32 devices in a mesh: dp: 2 (over x), fsdp: 4 (over z), ep: 4 (over y, core).
Axes of the slice: x: 2, y: 2, z: 4, core: 2. Of those that a mesh axis runs over, the one named last changes fastest.
Arguments:
- hidden: bfloat16 [65536, 4096], P(('dp', 'fsdp', 'ep')), parts along dimension 0
- norm_gain: bfloat16 [4096], replicated
- w_router: bfloat16 [4096, 8], replicated
- w_gate: bfloat16 [8, 4096, 1376], P('ep', 'fsdp')
- w_up: bfloat16 [8, 4096, 1376], P('ep', 'fsdp')
- w_down: bfloat16 [8, 1376, 4096], P('ep', None, 'fsdp')
- top2_ids: int32 [65536, 2], P(('dp', 'fsdp', 'ep')), parts along dimension 0
Outputs:
- output: bfloat16 [65536, 4096], P(('dp', 'fsdp', 'ep')), parts along dimension 0
There are 2 independent parts. The reference program is written for one: setup_inputs(seed, part) draws one part's arguments, and reference() takes and returns one part's arrays. A program takes and returns all parts, laid end to end along the dimension named above; an argument that names none is the same for every part.
All inputs are finite; a program needn't handle non-finite values.
Results may differ from the reference program's by a relative error of at most 0.001.
Values are sent between devices in bfloat16 or wider.
A program may use at most 1 GiB of HBM per device.

```python
import jax
import jax.numpy as jnp
import numpy as np
from jax import lax

D = 4096
FF = 1376
EXPERTS = 8
TOKENS_DEV = 2048
GROUPS = 16
TOKENS = GROUPS * TOKENS_DEV
CAPACITY = (5 * TOKENS_DEV + 2 * EXPERTS - 1) // (2 * EXPERTS)
EPS = 1e-5


def draw_routes(route_key):
    perm_key, first_key, second_key = jax.random.split(route_key, 3)
    hot_count = max(EXPERTS // 4, 1)
    route_table = jnp.asarray(np.repeat(np.arange(EXPERTS), np.where(np.arange(EXPERTS) < hot_count, 4, 1)), dtype=jnp.int32)
    expert_perm = jax.random.permutation(perm_key, EXPERTS)
    table_pick = jax.random.randint(first_key, (TOKENS,), 0, route_table.shape[0])
    local_index = jnp.arange(TOKENS, dtype=jnp.int32) % TOKENS_DEV
    first_choice = jnp.where(local_index < EXPERTS, local_index, expert_perm[route_table[table_pick]])
    second_shift = jax.random.randint(second_key, (TOKENS,), 1, EXPERTS)
    second_choice = (first_choice + second_shift) % EXPERTS
    return jnp.stack([first_choice, second_choice], axis=1).astype(jnp.int32)


def setup_inputs(seed: int = 0, part: int = 0) -> dict:
    part_key = jax.random.fold_in(jax.random.key(seed), part)
    hidden_key, route_key = jax.random.split(part_key, 2)
    gain_key, router_key, gate_key, up_key, down_key = jax.random.split(jax.random.key(seed + 1), 5)
    hidden = jax.random.normal(hidden_key, (TOKENS, D), jnp.float32)
    norm_gain = jax.random.uniform(gain_key, (D,), jnp.float32, 0.5, 1.5)
    w_router = jax.random.normal(router_key, (D, EXPERTS), jnp.float32) * (0.5 * D ** -0.5)
    w_gate = jax.random.normal(gate_key, (EXPERTS, D, FF), jnp.float32) * D ** -0.5
    w_up = jax.random.normal(up_key, (EXPERTS, D, FF), jnp.float32) * D ** -0.5
    w_down = jax.random.normal(down_key, (EXPERTS, FF, D), jnp.float32) * FF ** -0.5
    return {
        'hidden': hidden.astype(jnp.bfloat16),
        'norm_gain': norm_gain.astype(jnp.bfloat16),
        'w_router': w_router.astype(jnp.bfloat16),
        'w_gate': w_gate.astype(jnp.bfloat16),
        'w_up': w_up.astype(jnp.bfloat16),
        'w_down': w_down.astype(jnp.bfloat16),
        'top2_ids': draw_routes(route_key),
    }


def expert_ffn(expert_pack):
    rows_in, gate_mat, up_mat, down_mat = expert_pack
    act_a = jnp.dot(rows_in, gate_mat, preferred_element_type=jnp.float32)
    act_b = jnp.dot(rows_in, up_mat, preferred_element_type=jnp.float32)
    hidden_act = (jax.nn.silu(act_a) * act_b).astype(jnp.bfloat16)
    return jnp.dot(hidden_act, down_mat, preferred_element_type=jnp.float32).astype(jnp.bfloat16)


def reference(hidden, norm_gain, w_router, w_gate, w_up, w_down, top2_ids):
    hidden_f32 = hidden.astype(jnp.float32)
    mean_sq = jnp.mean(hidden_f32 * hidden_f32, axis=-1, keepdims=True)
    normed = (hidden_f32 * lax.rsqrt(mean_sq + EPS) * norm_gain.astype(jnp.float32)).astype(jnp.bfloat16)
    logits = jnp.dot(normed, w_router, preferred_element_type=jnp.float32)
    gate_probs = jax.nn.softmax(jnp.take_along_axis(logits, top2_ids, axis=1), axis=-1)
    flat_ids = top2_ids.reshape(GROUPS, 2 * TOKENS_DEV)
    onehot = (flat_ids[:, :, None] == jnp.arange(EXPERTS, dtype=jnp.int32)).astype(jnp.int32)
    position = jnp.sum((jnp.cumsum(onehot, axis=1) - 1) * onehot, axis=2)
    group_base = jnp.arange(GROUPS, dtype=jnp.int32)[:, None] * (EXPERTS * CAPACITY)
    all_slots = GROUPS * EXPERTS * CAPACITY
    slot_ids = jnp.where(position < CAPACITY, group_base + flat_ids * CAPACITY + position, all_slots).reshape(TOKENS, 2)
    token_index = jnp.broadcast_to(jnp.arange(TOKENS, dtype=jnp.int32)[:, None], (TOKENS, 2))
    source = jnp.full((all_slots,), TOKENS, dtype=jnp.int32).at[slot_ids.reshape(-1)].set(token_index.reshape(-1), mode='drop')
    buffers = jnp.take(normed, source, axis=0, mode='fill', fill_value=0)
    by_expert = buffers.reshape(GROUPS, EXPERTS, CAPACITY, D).transpose(1, 0, 2, 3).reshape(EXPERTS, GROUPS * CAPACITY, D)
    expert_out = lax.map(expert_ffn, (by_expert, w_gate, w_up, w_down))
    out_flat = expert_out.reshape(EXPERTS, GROUPS, CAPACITY, D).transpose(1, 0, 2, 3).reshape(all_slots, D)
    returned = jnp.take(out_flat, slot_ids, axis=0, mode='fill', fill_value=0)
    moe_sum = jnp.sum(gate_probs[:, :, None] * returned.astype(jnp.float32), axis=1)
    return (hidden_f32 + moe_sum).astype(jnp.bfloat16)
```

```python
import jax
import jax.numpy as jnp
from jax import lax
from jax.sharding import PartitionSpec as P

EPS = 1e-5


def norm_rows(hidden, norm_gain):
    hidden_f32 = hidden.astype(jnp.float32)
    mean_sq = jnp.mean(hidden_f32 * hidden_f32, axis=-1, keepdims=True)
    return (hidden_f32 * lax.rsqrt(mean_sq + EPS) * norm_gain.astype(jnp.float32)).astype(jnp.bfloat16)


def route_positions(top2_ids, num_experts, capacity):
    experts = jnp.arange(num_experts, dtype=jnp.int32)[:, None]
    chosen = (top2_ids[None, :, 0] == experts) | (top2_ids[None, :, 1] == experts)
    position = jnp.cumsum(chosen.astype(jnp.int32), axis=1) - 1
    return jnp.where(chosen & (position < capacity), position, -1)


def expert_gates(normed, w_router, top2_ids):
    logits = jnp.dot(normed, w_router, preferred_element_type=jnp.float32)
    experts = jnp.arange(w_router.shape[1], dtype=jnp.int32)[None, :]
    hit_0 = top2_ids[:, 0:1] == experts
    hit_1 = top2_ids[:, 1:2] == experts
    r_0 = jnp.sum(jnp.where(hit_0, logits, 0.0), axis=1, keepdims=True)
    r_1 = jnp.sum(jnp.where(hit_1, logits, 0.0), axis=1, keepdims=True)
    top = jnp.maximum(r_0, r_1)
    x_0, x_1 = jnp.exp(r_0 - top), jnp.exp(r_1 - top)
    total = x_0 + x_1
    return jnp.where(hit_0, x_0 / total, 0.0) + jnp.where(hit_1, x_1 / total, 0.0)


def pick_rows(slots_of_tokens, rows, capacity):
    slot = jnp.arange(capacity, dtype=jnp.int32)[:, None]
    select = (slots_of_tokens[None, :] == slot).astype(jnp.bfloat16)
    return jnp.dot(select, rows, preferred_element_type=jnp.float32).astype(jnp.bfloat16)


def expert_ffn(rows_in, gate_mat, up_mat, down_mat):
    act_a = jnp.dot(rows_in, gate_mat, preferred_element_type=jnp.float32)
    act_b = jnp.dot(rows_in, up_mat, preferred_element_type=jnp.float32)
    hidden_act = (jax.nn.silu(act_a) * act_b).astype(jnp.bfloat16)
    return jnp.dot(hidden_act, down_mat, preferred_element_type=jnp.float32).astype(jnp.bfloat16)


def local_block(hidden, norm_gain, w_router, w_gate, w_up, w_down, top2_ids):
    tok_local, d_model = hidden.shape
    num_experts = w_router.shape[1]
    capacity = (5 * tok_local + 2 * num_experts - 1) // (2 * num_experts)
    local_experts = w_gate.shape[0]
    ep_size = num_experts // local_experts
    me = lax.axis_index('ep')
    plane = lax.axis_index('dp')

    def swap(value, mask):
        return lax.ppermute(value, 'ep', [(i, i ^ mask) for i in range(ep_size)])

    def swap_plane(value):
        return lax.ppermute(value, 'dp', [(0, 1), (1, 0)])

    def after(value, *earlier):
        return lax.optimization_barrier((value,) + earlier)[0]

    shard = lax.axis_index('fsdp')
    shards = d_model // w_gate.shape[1]
    width = w_gate.shape[1]
    half = w_gate.shape[2] // 2

    def gather_own(w, unit_axis):
        part = lax.dynamic_slice_in_dim(w, plane * half, half, axis=unit_axis)
        return lax.all_gather(part, 'fsdp', axis=1 - unit_axis, tiled=True)

    def exchange(own, w, unit_axis):
        d_axis = 1 - unit_axis
        other = lax.dynamic_slice_in_dim(w, (1 - plane) * half, half, axis=unit_axis)
        pieces = [(shard, other)]
        for k in range(1, shards):
            at = (shard + k) % shards
            block = lax.dynamic_slice_in_dim(own, at * width, width, axis=d_axis)
            pieces.append((at, swap_plane(block)))
        return pieces

    def assemble(own, pieces, unit_axis):
        full = lax.concatenate([own, own], unit_axis)
        for at, piece in pieces:
            start = (at * width, half) if unit_axis == 1 else (half, at * width)
            full = lax.dynamic_update_slice(full, piece, start)
        return full

    normed = norm_rows(hidden, norm_gain)
    far = swap(normed, 2)
    near = swap(normed, 1)
    positions = route_positions(top2_ids, num_experts, capacity)
    slots = [positions] + [swap(positions, m) for m in range(1, ep_size)]
    gates = expert_gates(normed, w_router, top2_ids)

    owns = []
    for i in range(local_experts):
        for w, unit_axis in ((w_gate, 1), (w_up, 1), (w_down, 0)):
            own = gather_own(w[i], unit_axis)
            owns.append((own, w[i], unit_axis))

    def weights_of(i, *earlier):
        full = []
        for own, w, unit_axis in owns[3 * i:3 * i + 3]:
            if earlier:
                own = after(own, *earlier)
            full.append(assemble(own, exchange(own, w, unit_axis), unit_axis))
        return full

    def at_expert(i, m):
        return lax.dynamic_index_in_dim(slots[m], local_experts * me + i, 0, keepdims=False)

    def pick(i, m, source):
        return pick_rows(at_expert(i, m), source, capacity)

    slot_row = jnp.arange(capacity, dtype=jnp.int32)[None, :]

    def add_back(*args):
        return lax.optimization_barrier(combine(*args))

    def combine(total, i, m, back):
        expert = local_experts * (me ^ m) + i
        mine = lax.dynamic_index_in_dim(positions, expert, 0, keepdims=False)
        gate = lax.dynamic_index_in_dim(gates, expert, 1, keepdims=True)
        select = (mine[:, None] == slot_row).astype(jnp.bfloat16)
        return total + gate * jnp.dot(select, back, preferred_element_type=jnp.float32)

    picked = {}
    for i in range(local_experts):
        picked[i, 0] = pick(i, 0, normed)
        picked[i, 1] = pick(i, 1, near)
    first = weights_of(0)
    relay = swap(far, 1)
    order = (2, 3, 1, 0)
    outs, backs = {}, {}
    picked[0, 2] = pick(0, 2, far)
    done = None
    for m in order:
        if m == 3:
            picked[0, 3] = pick(0, 3, after(relay, done))
        rows_in = picked[0, m] if done is None else after(picked[0, m], done)
        done = expert_ffn(rows_in, *first)
        outs[0, m] = done
        backs[0, m] = swap(done, m) if m else done
        if m == 2:
            second = weights_of(1, done)
    picked[1, 2] = pick(1, 2, after(far, done))
    picked[1, 3] = pick(1, 3, after(relay, done))
    total = hidden.astype(jnp.float32)
    total = add_back(total, 0, 0, after(backs[0, 0], picked[1, 2], picked[1, 3]))
    total = add_back(total, 0, 1, backs[0, 1])
    for m in order:
        done = expert_ffn(after(picked[1, m], done, total), *second)
        backs[1, m] = swap(done, m) if m else done
    total = add_back(total, 1, 0, backs[1, 0])
    total = add_back(total, 0, 2, backs[0, 2])
    total = add_back(total, 1, 1, backs[1, 1])
    total = add_back(total, 0, 3, backs[0, 3])
    total = add_back(total, 1, 2, backs[1, 2])
    total = combine(total, 1, 3, backs[1, 3])
    return total.astype(jnp.bfloat16)


def solution(mesh):
    tok_spec = P(('dp', 'fsdp', 'ep'), None)
    in_specs = (tok_spec, P(None), P(None, None), P('ep', 'fsdp', None), P('ep', 'fsdp', None), P('ep', None, 'fsdp'), tok_spec)
    return jax.shard_map(local_block, mesh=mesh, in_specs=in_specs, out_specs=tok_spec, check_vma=False)
```

```python
import functools

import jax
import jax.numpy as jnp
from jax import lax
from jax.experimental import pallas as pl
from jax.experimental.pallas import tpu as pltpu
from jax.sharding import PartitionSpec as P

EPS = 1e-5
CHUNK = 256
WINDOW = 128
SPAN = 160
BUFFERS = 4
VMEM_LIMIT = 63 * 1024 * 1024
NT = (((1,), (1,)), ((), ()))


def norm_rows(hidden, norm_gain):
    hidden_f32 = hidden.astype(jnp.float32)
    mean_sq = jnp.mean(hidden_f32 * hidden_f32, axis=-1, keepdims=True)
    return (hidden_f32 * lax.rsqrt(mean_sq + EPS) * norm_gain.astype(jnp.float32)).astype(jnp.bfloat16)


def expert_gates(normed, w_router, top2_ids, order):
    logits = jnp.dot(normed, w_router, preferred_element_type=jnp.float32)
    experts = jnp.arange(w_router.shape[1], dtype=jnp.int32)[None, :]
    hit_0 = top2_ids[:, 0:1] == experts
    hit_1 = top2_ids[:, 1:2] == experts
    r_0 = jnp.sum(jnp.where(hit_0, logits, 0.0), axis=1, keepdims=True)
    r_1 = jnp.sum(jnp.where(hit_1, logits, 0.0), axis=1, keepdims=True)
    top = jnp.maximum(r_0, r_1)
    x_0, x_1 = jnp.exp(r_0 - top), jnp.exp(r_1 - top)
    total = x_0 + x_1
    at_0, at_1 = top2_ids[:, 0:1] == order, top2_ids[:, 1:2] == order
    return jnp.where(at_0, x_0 / total, 0.0) + jnp.where(at_1, x_1 / total, 0.0)


def slots_and_bounds(chosen, capacity):
    count = jnp.cumsum(chosen.astype(jnp.int32), axis=1)
    slots = jnp.where(chosen & (count <= capacity), count - 1, -1)
    ends = jnp.minimum(count[:, CHUNK - 1::CHUNK], capacity)
    bounds = jnp.concatenate([jnp.zeros((ends.shape[0], 1), jnp.int32), ends], axis=1)
    return slots, bounds


def ffn_kernel(expert, row, capacity, shards, table, slots, gain, hid, gate_arg, up_arg, gate_own, g1, g2, g3,
               up_own, u1, u2, u3, down, out, weights, rows, hid_buf, act, hid_sem, w_sem):
    d_model = hid.shape[1]
    chunks = hid.shape[0] // CHUNK
    half, width = g1.shape
    units = 2 * half
    shard = table[row, chunks + 1]
    plane = table[row, chunks + 2]
    mine = pl.multiple_of(plane * half, 16)
    theirs = pl.multiple_of((1 - plane) * half, 16)

    def load_chunk(c):
        return pltpu.make_async_copy(hid.at[pl.ds(c * CHUNK, CHUNK), :], hid_buf.at[c % BUFFERS], hid_sem.at[c % BUFFERS])

    copies = []
    for w, (arg, own, others) in enumerate(((gate_arg, gate_own, (g1, g2, g3)), (up_arg, up_own, (u1, u2, u3)))):
        group = [pltpu.make_async_copy(own, weights.at[w, pl.ds(mine, half), :], w_sem.at[w])]
        col = pl.multiple_of(shard * width, 128)
        group.append(pltpu.make_async_copy(
            arg.at[expert, pl.ds(theirs, half), :], weights.at[w, pl.ds(theirs, half), pl.ds(col, width)], w_sem.at[w]))
        for k, other in enumerate(others):
            col = pl.multiple_of(((shard + k + 1) % shards) * width, 128)
            group.append(pltpu.make_async_copy(
                other, weights.at[w, pl.ds(theirs, half), pl.ds(col, width)], w_sem.at[w]))
        copies.append(group)
    copies.append([pltpu.make_async_copy(down, weights.at[2], w_sem.at[2])])

    for c in range(BUFFERS):
        load_chunk(c).start()
    for group in copies:
        for copy in group:
            copy.start()

    rows[...] = jnp.zeros_like(rows)
    for c in range(chunks):
        load_chunk(c).wait()
        low, high = table[row, c], table[row, c + 1]
        base = low // 16 * 16

        def pick(w, carry, c=c, base=base):
            start = pl.multiple_of(base + w * WINDOW, 16)
            slot = lax.broadcasted_iota(jnp.int32, (WINDOW, CHUNK), 0) + start
            select = (slots[row * chunks + c:row * chunks + c + 1, :] == slot).astype(jnp.float32).astype(jnp.bfloat16)

            def column(n, carry):
                at = pl.ds(pl.multiple_of(n * 1024, 1024), 1024)
                got = jnp.dot(select, hid_buf[c % BUFFERS, :, at], preferred_element_type=jnp.float32)
                held = rows[pl.ds(start, WINDOW), at].astype(jnp.float32)
                rows[pl.ds(start, WINDOW), at] = (held + got).astype(jnp.bfloat16)
                return carry

            return lax.fori_loop(0, d_model // 1024, column, carry)

        lax.fori_loop(0, (high - base + WINDOW - 1) // WINDOW, pick, 0)
        if c + BUFFERS < chunks:
            load_chunk(c + BUFFERS).start()

    def norm(b, carry):
        at = pl.ds(pl.multiple_of(b * 32, 32), 32)
        x = rows[at, :].astype(jnp.float32)
        mean_sq = jnp.mean(x * x, axis=-1, keepdims=True)
        rows[at, :] = (x * lax.rsqrt(mean_sq + EPS) * gain[...].astype(jnp.float32)).astype(jnp.bfloat16)
        return carry

    lax.fori_loop(0, capacity // 32, norm, 0)
    for group in copies[:2]:
        for copy in group:
            copy.wait()

    def hidden_units(at):
        x = rows[0:capacity, :]
        a = lax.dot_general(x, weights[0, at, :], NT, preferred_element_type=jnp.float32)
        b = lax.dot_general(x, weights[1, at, :], NT, preferred_element_type=jnp.float32)
        act[:, at] = (a * (1.0 / (1.0 + jnp.exp(-a))) * b).astype(jnp.bfloat16)

    tiles = units // 256

    def tile(t, carry):
        hidden_units(pl.ds(pl.multiple_of(t * 256, 256), 256))
        return carry

    lax.fori_loop(0, tiles, tile, 0)
    if units % 256:
        hidden_units(pl.ds(tiles * 256, units % 256))
    for copy in copies[2]:
        copy.wait()

    def project(n, carry):
        at = pl.ds(pl.multiple_of(n * 512, 512), 512)
        out[:, at] = jnp.dot(act[...], weights[2, :, at], preferred_element_type=jnp.float32).astype(jnp.bfloat16)
        return carry

    lax.fori_loop(0, d_model // 512, project, 0)


def expert_ffn(expert, row, capacity, table, slots, gain, hid, gate_arg, up_arg, gate, up, down):
    tokens, d_model = hid.shape
    units = 2 * gate[0].shape[0]
    shards = d_model // gate[1].shape[1]
    any_spec = pl.BlockSpec(memory_space=pl.ANY)
    vmem_spec = pl.BlockSpec(memory_space=pltpu.VMEM)
    return pl.pallas_call(
        functools.partial(ffn_kernel, expert, row, capacity, shards),
        out_shape=jax.ShapeDtypeStruct((capacity, d_model), jnp.bfloat16),
        in_specs=[pl.BlockSpec(memory_space=pltpu.SMEM), vmem_spec, vmem_spec] + [any_spec] * 12,
        out_specs=vmem_spec,
        scratch_shapes=[
            pltpu.VMEM((3, units, d_model), jnp.bfloat16),
            pltpu.VMEM((capacity + WINDOW, d_model), jnp.bfloat16),
            pltpu.VMEM((BUFFERS, CHUNK, d_model), jnp.bfloat16),
            pltpu.VMEM((capacity, units), jnp.bfloat16),
            pltpu.SemaphoreType.DMA((BUFFERS,)),
            pltpu.SemaphoreType.DMA((3,)),
        ],
        compiler_params=pltpu.CompilerParams(vmem_limit_bytes=VMEM_LIMIT),
        cost_estimate=pl.CostEstimate(flops=6 * capacity * d_model * units, transcendentals=capacity * units,
                                      bytes_accessed=2 * (3 * units + tokens + capacity) * d_model),
    )(table, slots, gain.reshape(1, d_model), hid, gate_arg, up_arg, *gate, *up, down)


def combine_kernel(capacity, first_row, count, bounds, base_ref, slots, gates, *refs):
    sources, out, acc, buf, sem = refs[:count], refs[count], refs[count + 1], refs[count + 2], refs[count + 3]
    b = pl.program_id(0)
    steps = pl.num_programs(0)
    d_model = acc.shape[1]

    def begin(step, k, w):
        low = bounds[first_row + k, step]
        return jnp.minimum(low // 16 * 16 + w * SPAN, capacity - SPAN)

    def load(step, k, w, slot):
        start = pl.multiple_of(begin(step, k, w), 16)
        return pltpu.make_async_copy(sources[k].at[pl.ds(start, SPAN), :], buf.at[slot, k], sem.at[slot, k])

    @pl.when(b == 0)
    def _():
        for k in range(count):
            load(0, k, 0, 0).start()

    @pl.when(b + 1 < steps)
    def _():
        for k in range(count):
            load(b + 1, k, 0, (b + 1) % 2).start()

    acc[...] = base_ref[...].astype(jnp.float32)
    here = b % 2
    for k in range(count):
        load(b, k, 0, here).wait()
        first = bounds[first_row + k, b] // 16 * 16

        def add(w, carry, k=k, first=first):
            @pl.when(w > 0)
            def _():
                again = load(b, k, w, here)
                again.start()
                again.wait()

            mine = slots[:, first_row + k:first_row + k + 1]
            mine = jnp.where(mine >= first + w * SPAN, mine - begin(b, k, w), -1)
            select = (mine == lax.broadcasted_iota(jnp.int32, (CHUNK, SPAN), 1)).astype(jnp.float32).astype(jnp.bfloat16)
            gate = gates[:, first_row + k:first_row + k + 1]

            def column(n, carry):
                at = pl.ds(pl.multiple_of(n * 512, 512), 512)
                acc[:, at] += gate * jnp.dot(select, buf[here, k, :, at], preferred_element_type=jnp.float32)
                return carry

            return lax.fori_loop(0, d_model // 512, column, carry)

        windows = (bounds[first_row + k, b + 1] - first + SPAN - 1) // SPAN
        lax.fori_loop(0, windows, add, 0)
    out[...] = acc[...].astype(out.dtype)


def combine(capacity, first_row, base, slots, gates, bounds, sources, out_dtype):
    tokens, d_model = base.shape
    count = len(sources)
    rows = pl.BlockSpec((CHUNK, d_model), lambda b, *_: (b, 0))
    small = pl.BlockSpec((CHUNK, slots.shape[1]), lambda b, *_: (b, 0))
    return pl.pallas_call(
        functools.partial(combine_kernel, capacity, first_row, count),
        out_shape=jax.ShapeDtypeStruct((tokens, d_model), out_dtype),
        grid_spec=pltpu.PrefetchScalarGridSpec(
            num_scalar_prefetch=1,
            grid=(tokens // CHUNK,),
            in_specs=[rows, small, small] + [pl.BlockSpec(memory_space=pl.ANY)] * count,
            out_specs=rows,
            scratch_shapes=[
                pltpu.VMEM((CHUNK, d_model), jnp.float32),
                pltpu.VMEM((2, count, SPAN, d_model), jnp.bfloat16),
                pltpu.SemaphoreType.DMA((2, count)),
            ]),
        compiler_params=pltpu.CompilerParams(vmem_limit_bytes=VMEM_LIMIT, dimension_semantics=("arbitrary",)),
        cost_estimate=pl.CostEstimate(flops=4 * tokens * SPAN * d_model * count, transcendentals=0,
                                      bytes_accessed=tokens * d_model * (4 + 2 * count)),
    )(bounds, base, slots, gates, *sources)


def local_block(hidden, norm_gain, w_router, w_gate, w_up, w_down, top2_ids):
    tok_local, d_model = hidden.shape
    num_experts = w_router.shape[1]
    capacity = (5 * tok_local + 2 * num_experts - 1) // (2 * num_experts)
    local_experts = w_gate.shape[0]
    ep_size = num_experts // local_experts
    me = lax.axis_index('ep')
    plane = lax.axis_index('dp')
    shard = lax.axis_index('fsdp')
    width = w_gate.shape[1]
    shards = d_model // width
    half = w_gate.shape[2] // 2

    def swap(value, mask):
        return lax.ppermute(value, 'ep', [(i, i ^ mask) for i in range(ep_size)])

    def swap_plane(value):
        return lax.ppermute(value, 'dp', [(0, 1), (1, 0)])

    def after(value, *earlier):
        return lax.optimization_barrier((value,) + earlier)[0]

    ids = top2_ids.T
    ids_of = [ids] + [swap(ids, m) for m in range(1, ep_size)]
    tokens = after(hidden, *ids_of)
    near = swap(tokens, 1)
    far = swap(tokens, 2)

    gate_t = w_gate.transpose(0, 2, 1)
    up_t = w_up.transpose(0, 2, 1)

    def gather_own(w_t, i):
        part = lax.dynamic_slice(w_t, (i, plane * half, 0), (1, half, width))[0]
        return lax.all_gather(part, 'fsdp', axis=1, tiled=True)

    def gather_both(w, i):
        part = lax.dynamic_slice(w, (i, 0, plane * (width // 2)), (1, w.shape[1], width // 2))[0]
        return lax.all_gather(part, ('fsdp', 'dp'), axis=1, tiled=True)

    def exchange(own):
        at = [(shard + k) % shards * width for k in range(1, shards)]
        return [own] + [swap_plane(lax.dynamic_slice_in_dim(own, start, width, axis=1)) for start in at]

    own = []
    for i in range(local_experts):
        own.append((gather_own(gate_t, i), gather_own(up_t, i), gather_both(w_down, i)))

    all_ids = jnp.concatenate(ids_of, axis=0).reshape(ep_size, 1, 2, tok_local)
    here = (local_experts * me + jnp.arange(local_experts, dtype=jnp.int32))[None, :, None]
    chosen = (all_ids[:, :, 0] == here) | (all_ids[:, :, 1] == here)
    slots, bounds = slots_and_bounds(chosen.reshape(num_experts, tok_local), capacity)
    slots = slots.reshape(num_experts * (tok_local // CHUNK), CHUNK)
    place = jnp.broadcast_to(jnp.stack([shard, plane]).astype(jnp.int32)[None, :], (num_experts, 2))
    tables = jnp.concatenate([bounds, place], axis=1)
    back = jnp.arange(num_experts, dtype=jnp.int32)
    back = local_experts * (me ^ (back % ep_size)) + back // ep_size
    chosen = (ids[0:1] == back[:, None]) | (ids[1:2] == back[:, None])
    back_slots, back_bounds = slots_and_bounds(chosen, capacity)
    back_slots = back_slots.T
    back_gates = expert_gates(norm_rows(hidden, norm_gain), w_router, top2_ids, back[None, :])
    tokens_of = [hidden, near, far, None]

    def run(i, m, weights, *earlier):
        row = m * local_experts + i
        hid = tokens_of[m] if not earlier else after(tokens_of[m], *earlier)
        out = expert_ffn(i, row, capacity, tables, slots, norm_gain, hid, gate_t, up_t, *weights)
        if not m:
            return out, out
        return out, swap(out, m)

    def put(base, i, m, backs, dtype):
        return combine(capacity, i * ep_size + m, base, back_slots, back_gates, back_bounds, backs, dtype)

    gate_a, up_a, down_a = own[0]
    weights = exchange(gate_a), exchange(up_a), down_a
    tokens_of[3] = swap(after(far, near, slots, tables, *weights[0][1:], *weights[1][1:]), 1)
    out_2, back_2 = run(0, 2, weights)
    out_3, back_3 = run(0, 3, weights, out_2)
    out_1, back_1 = run(0, 1, weights, out_3)
    out_0, back_0 = run(0, 0, weights, out_1)

    gate_b, up_b, down_b = own[1]
    weights = exchange(after(gate_b, out_0)), exchange(after(up_b, out_0))
    total = put(hidden, 0, 0, [back_0, back_1, back_2, back_3], jnp.float32)
    weights = weights + (after(down_b, total),)
    out_2, back_2 = run(1, 2, weights)
    out_3, back_3 = run(1, 3, weights, out_2)
    out_1, back_1 = run(1, 1, weights, out_3)
    out_0, back_0 = run(1, 0, weights, out_1)
    total = put(total, 1, 0, [back_0, back_1], jnp.float32)
    return put(total, 1, 2, [back_2, back_3], jnp.bfloat16)


def solution(mesh):
    tok_spec = P(('dp', 'fsdp', 'ep'), None)
    in_specs = (tok_spec, P(None), P(None, None), P('ep', 'fsdp', None), P('ep', 'fsdp', None), P('ep', None, 'fsdp'), tok_spec)
    return jax.shard_map(local_block, mesh=mesh, in_specs=in_specs, out_specs=tok_spec, check_vma=False)
```
